32 devices in a mesh: dp: 4 (over z), tp: 8 (over y, x, core).
Axes of the slice: x: 2, y: 2, z: 4, core: 2. Of those that a mesh axis runs over, the one named last changes fastest.
Arguments:
- ids: int32 [32, 256], P('dp'), parts along dimension 0
- E: bfloat16 [16384, 3072], P('tp')
- g: bfloat16 [3072], replicated
- W: bfloat16 [3072, 5120], P(None, 'tp')
- du: bfloat16 [32, 256, 5120], P('dp', None, 'tp'), parts along dimension 0
- dres: bfloat16 [32, 256, 3072], P('dp', 'tp'), parts along dimension 0
Outputs:
- output 1: bfloat16 [32, 256, 5120], P('dp', None, 'tp'), parts along dimension 0
- output 2: bfloat16 [32, 256, 3072], P('dp', 'tp'), parts along dimension 0
- output 3: float32 [65536, 3072], P(('dp', 'tp')), parts along dimension 0
- output 4: float32 [12288, 5120], P('dp', 'tp'), parts along dimension 0
- output 5: float32 [12288], P('dp'), parts along dimension 0
There are 4 independent parts. The reference program is written for one: setup_inputs(seed, part) draws one part's arguments, and reference() takes and returns one part's arrays. A program takes and returns all parts, laid end to end along the dimension named above; an argument that names none is the same for every part.
All inputs are finite; a program needn't handle non-finite values.
Results may differ from the reference program's by a relative error of at most 0.00687744.
Values are sent between devices in bfloat16 or wider.
A program may use at most 1 GiB of HBM per device.

```python
import jax
import jax.numpy as jnp
from jax import lax

V = 16384
K = 8
T = 256
D = 3072
FC = 5120
TP = 8
NPOP = 256
EPS = 1e-6


def setup_inputs(seed: int = 0, part: int = 0) -> dict:
    key = jax.random.key(seed)
    kp = jax.random.fold_in(key, part)
    k1, k2, k3, k4, k5, k6 = jax.random.split(kp, 6)
    s1, s2, s3 = jax.random.split(key, 3)
    kd = jax.random.fold_in(kp, 7)
    d1, d2, d3, d4 = jax.random.split(kd, 4)
    vs = V // TP
    pop = jnp.arange(TP, dtype=jnp.int32) * vs + jax.random.randint(d1, (TP,), 0, vs, dtype=jnp.int32)
    pick = jax.random.randint(d2, (K, T), 0, TP, dtype=jnp.int32)
    uni = jax.random.randint(d3, (K, T), 0, V, dtype=jnp.int32)
    coin = jax.random.bernoulli(d4, 0.75, (K, T))
    ids = jnp.where(coin, pop[pick], uni).astype(jnp.int32)
    E = jax.random.normal(s1, (V, D), jnp.float32).astype(jnp.bfloat16)
    g = (1.0 + 0.4 * jax.random.normal(s2, (D,), jnp.float32)).astype(jnp.bfloat16)
    W = (jax.random.normal(s3, (D, FC), jnp.float32) * D ** -0.5).astype(jnp.bfloat16)
    du = jax.random.normal(k5, (K, T, FC), jnp.float32).astype(jnp.bfloat16)
    dres = jax.random.normal(k6, (K, T, D), jnp.float32).astype(jnp.bfloat16)
    return {"ids": ids, "E": E, "g": g, "W": W, "du": du, "dres": dres}


def reference(ids, E, g, W, du, dres):
    gf = g.astype(jnp.float32)
    fs = FC // TP
    wr = W.reshape(D, TP, fs).transpose(1, 0, 2)

    def micro(carry, inp):
        dE, dW, dg = carry
        idk, duk, dresk = inp
        x = jnp.take(E, idk, axis=0)
        xf = x.astype(jnp.float32)
        rs = lax.rsqrt(jnp.mean(xf * xf, axis=-1, keepdims=True) + EPS)
        nh = xf * rs
        n = (nh * gf).astype(jnp.bfloat16)
        u = jnp.dot(n, W, preferred_element_type=jnp.float32).astype(jnp.bfloat16)
        dur = duk.reshape(T, TP, fs).transpose(1, 0, 2)

        def add_block(acc, blk):
            dub, wb = blk
            pr = jnp.dot(dub, wb.T, preferred_element_type=jnp.float32)
            return acc + pr.astype(jnp.bfloat16).astype(jnp.float32), None

        dn, _ = lax.scan(add_block, jnp.zeros((T, D), jnp.float32), (dur, wr))
        gdn = gf * dn
        dx = dresk.astype(jnp.float32) + rs * (gdn - nh * jnp.mean(nh * gdn, axis=-1, keepdims=True))
        dxb = dx.astype(jnp.bfloat16).astype(jnp.float32)
        dE = dE.at[idk].add(dxb)
        dW = dW + jnp.dot(n.T, duk, preferred_element_type=jnp.float32)
        dg = dg + jnp.sum(dn * nh, axis=0)
        return (dE, dW, dg), (u, x)

    init = (jnp.zeros((V, D), jnp.float32), jnp.zeros((D, FC), jnp.float32), jnp.zeros((D,), jnp.float32))
    (dE, dW, dg), (u, x) = lax.scan(micro, init, (ids, du, dres))
    return u, x, dE, dW, dg
```

```python
import jax
import jax.numpy as jnp
from jax import lax
from jax.sharding import PartitionSpec as P

EPS = 1e-6
CX = 96
CD = 24

C0 = (((0,), (0,)), ((), ()))
C1 = (((1,), (1,)), ((), ()))
F32 = jnp.float32
BF16 = jnp.bfloat16


def rnd(v):
    return lax.reduce_precision(v, 8, 7)


def solution(mesh):
    ntp = mesh.shape["tp"]

    def pp(v, j):
        return lax.ppermute(v, "tp", [(i, i ^ j) for i in range(ntp)])

    def grad_dx(dn, xl, gf, dresl):
        xf = xl.astype(F32)
        rs = lax.rsqrt(jnp.mean(xf * xf, axis=-1, keepdims=True) + EPS)
        nh = xf * rs
        gdn = gf * dn
        dx = dresl.astype(F32) + rs * (gdn - nh * jnp.mean(nh * gdn, axis=-1, keepdims=True))
        dg = jnp.sum(dn * nh, axis=0)
        return dx.astype(BF16), dg

    def body(ids, E, g, W, du, dres):
        vs, d = E.shape
        nk, t = ids.shape
        ts = t // ntp
        nt = nk * t
        fs = W.shape[1]
        h = d // 2
        me = lax.axis_index("tp")
        core = me & 1
        chip = me >> 1
        lo = me * vs
        gf = g.astype(F32)

        idf = ids.reshape(nt)
        own = idf // vs
        tok = jnp.arange(nt, dtype=jnp.int32)
        big = jnp.int32(1 << 20)
        eq = idf[:, None] == idf[None, :]
        first = jnp.min(jnp.where(eq, tok[:, None], big), axis=0)
        isf = first == tok
        slot = jnp.sum(
            (isf[:, None] & (own[:, None] == own[None, :]) & (tok[:, None] < first[None, :])).astype(jnp.int32), axis=0
        )
        idl = ids.reshape(nk, ntp, ts).transpose(1, 0, 2).reshape(ntp, nk * ts)
        ownl = idl // vs
        tl = jnp.arange(nk * ts, dtype=jnp.int32)
        eql = idl[:, :, None] == idl[:, None, :]
        firstl = jnp.min(jnp.where(eql, tl[None, :, None], big), axis=1)
        isfl = firstl == tl[None, :]
        slotl = jnp.sum(
            (
                isfl[:, :, None] & (ownl[:, :, None] == ownl[:, None, :]) & (tl[None, :, None] < firstl[:, None, :])
            ).astype(jnp.int32),
            axis=1,
        )
        over = (jnp.max(slot) >= CX) | (jnp.max(slotl) >= CD)

        def rel(o):
            return ((o ^ me) & 1) * (ntp // 2) + ((o ^ me) >> 1)

        duv = du.reshape(nk, ntp // 2, 2, ts, fs)
        dum = lax.dynamic_index_in_dim(duv, core, 2, keepdims=False)
        dut = lax.dynamic_index_in_dim(duv, 1 - core, 2, keepdims=False)
        dus = pp(dut, 1)
        ws = pp(W, 1)

        def fast(ids, E, g, W, du, dres, ws, dus, dum):
            row_of = jnp.max(
                jnp.where(
                    (own == me)[:, None] & (slot[:, None] == jnp.arange(CX, dtype=jnp.int32)[None, :]),
                    (idf - lo)[:, None],
                    -1,
                ),
                axis=0,
            )
            ohe = (row_of[:, None] == lax.broadcasted_iota(jnp.int32, (CX, vs), 1)).astype(BF16)
            xc = jnp.dot(ohe, E, preferred_element_type=F32).astype(BF16)
            hc = CX // 2
            px = pp(xc, 2)
            py = pp(xc, 4)
            dlo = pp(px[:hc], 4)
            dhi = pp(py[hc:], 2)
            xh = jnp.concatenate([xc, px, py, dlo, dhi], axis=0)
            xall = jnp.concatenate([xh, pp(xh, 1)], axis=0)
            xf = xall.astype(F32)
            rs = lax.rsqrt(jnp.mean(xf * xf, axis=-1, keepdims=True) + EPS)
            nc = (xf * rs * gf).astype(BF16)
            gpos = rel(own) * CX + slot
            oh = (gpos[:, None] == lax.broadcasted_iota(jnp.int32, (nt, ntp * CX), 1)).astype(BF16)
            n = jnp.dot(oh, nc, preferred_element_type=F32).astype(BF16)
            u = jnp.dot(n, W, preferred_element_type=F32).astype(BF16).reshape(nk, t, fs)
            dW = lax.dot_general(n, du.reshape(nt, fs), C0, preferred_element_type=F32)
            ohl = lax.dynamic_slice_in_dim(oh.reshape(nk, t, ntp * CX), me * ts, ts, 1).reshape(nk * ts, ntp * CX)
            xl = jnp.dot(ohl, xall, preferred_element_type=F32).astype(BF16)

            def p2(k):
                q = chip ^ k
                a = lax.dynamic_index_in_dim(dum, q, 1, keepdims=False).reshape(nk * ts, fs)
                b = lax.dynamic_index_in_dim(dus, q, 1, keepdims=False).reshape(nk * ts, fs)
                pa = rnd(lax.dot_general(a, W, C1, preferred_element_type=F32))
                pb = rnd(lax.dot_general(b, ws, C1, preferred_element_type=F32))
                return pa + pb

            p3 = p2(3)
            r2 = pp(p3[:, :h], 2)
            r1 = pp(p3[:, h:], 4)
            p1 = p2(1)
            p2_ = p2(2)
            ax = pp(p1[:, :h], 2)
            ay = pp(p2_[:, h:], 4)
            p0 = p2(0)
            by = pp(p2_[:, :h] + r2, 4)
            bx = pp(p1[:, h:] + r1, 2)
            dn = jnp.concatenate([p0[:, :h] + ax + by, p0[:, h:] + ay + bx], axis=1)

            dxb, dg = grad_dx(dn, xl, gf, dres.reshape(nk * ts, d))
            for j in (1, 2, 4):
                dg = dg + pp(dg, j)

            idm = lax.dynamic_index_in_dim(idl, me, 0, keepdims=False)
            om = idm // vs
            sm = lax.dynamic_index_in_dim(slotl, me, 0, keepdims=False)
            pm = (om ^ me) * CD + sm
            ohm = (lax.broadcasted_iota(jnp.int32, (ntp * CD, nk * ts), 0) == pm[None, :]).astype(BF16)
            rows = jnp.dot(ohm, dxb, preferred_element_type=F32).reshape(ntp, CD, d)
            got = jnp.concatenate([rows[0]] + [pp(rows[j], j) for j in range(1, ntp)], axis=0)
            vr = jnp.max(
                jnp.where(
                    (ownl == me)[:, :, None] & (slotl[:, :, None] == jnp.arange(CD, dtype=jnp.int32)[None, None, :]),
                    (idl - lo)[:, :, None],
                    -1,
                ),
                axis=1,
            )
            vr = jnp.take(vr, jnp.arange(ntp, dtype=jnp.int32) ^ me, axis=0).reshape(ntp * CD)
            s1 = rnd(got)
            e1 = got - s1
            s2 = rnd(e1)
            s3 = e1 - s2
            sp = jnp.concatenate([s1.astype(BF16), s2.astype(BF16), s3.astype(BF16)], axis=0)
            vr3 = jnp.concatenate([vr, vr, vr], axis=0)
            ohd = (lax.broadcasted_iota(jnp.int32, (vs, 3 * ntp * CD), 0) == vr3[None, :]).astype(BF16)
            dE = jnp.dot(ohd, sp, preferred_element_type=F32)
            return u, xl.reshape(nk, ts, d), dE, dW, dg

        def slow(ids, E, g, W, du, dres, ws, dus, dum):
            oh = (lax.broadcasted_iota(jnp.int32, (vs, nt), 0) == (idf - lo)[None, :]).astype(BF16)
            x = lax.dot_general(oh, E, C0, preferred_element_type=F32).astype(BF16)
            for j in (1, 2, 4):
                x = x + pp(x, j)
            xf = x.astype(F32)
            rs = lax.rsqrt(jnp.mean(xf * xf, axis=-1, keepdims=True) + EPS)
            n = (xf * rs * gf).astype(BF16)
            u = jnp.dot(n, W, preferred_element_type=F32).astype(BF16).reshape(nk, t, fs)
            dW = lax.dot_general(n, du.reshape(nt, fs), C0, preferred_element_type=F32)
            xl = lax.dynamic_slice_in_dim(x.reshape(nk, t, d), me * ts, ts, 1).reshape(nk * ts, d)
            p = lax.dot_general(du.reshape(nt, fs), W, C1, preferred_element_type=F32).astype(BF16)
            p = p.reshape(nk, ntp, ts, d)
            dn = jnp.zeros((nk * ts, d), F32)
            for j in range(ntp):
                q = lax.dynamic_index_in_dim(p, me ^ j, 1, keepdims=False).reshape(nk * ts, d)
                if j:
                    q = pp(q, j)
                dn = dn + q.astype(F32)
            dxb, dg = grad_dx(dn, xl, gf, dres.reshape(nk * ts, d))
            for j in (1, 2, 4):
                dg = dg + pp(dg, j)
            dE = jnp.zeros((vs, d), F32)
            for j in range(ntp):
                q = pp(dxb, j) if j else dxb
                iq = lax.dynamic_index_in_dim(idl, me ^ j, 0, keepdims=False)
                ohq = (lax.broadcasted_iota(jnp.int32, (vs, nk * ts), 0) == (iq - lo)[None, :]).astype(BF16)
                dE = dE + jnp.dot(ohq, q, preferred_element_type=F32)
            return u, xl.reshape(nk, ts, d), dE, dW, dg

        return lax.cond(over, slow, fast, ids, E, g, W, du, dres, ws, dus, dum)

    return jax.shard_map(
        body,
        mesh=mesh,
        in_specs=(P("dp", None), P("tp", None), P(None), P(None, "tp"), P("dp", None, "tp"), P("dp", "tp", None)),
        out_specs=(P("dp", None, "tp"), P("dp", "tp", None), P(("dp", "tp"), None), P("dp", "tp"), P("dp")),
        check_vma=False,
    )
```

```python
import jax
import jax.numpy as jnp
from jax import lax
from jax.sharding import PartitionSpec as P

EPS = 1e-6
CX = 96
CD = 24

C0 = (((0,), (0,)), ((), ()))
C1 = (((1,), (1,)), ((), ()))
F32 = jnp.float32
BF16 = jnp.bfloat16


def rnd(v):
    return lax.reduce_precision(v, 8, 7)


def solution(mesh):
    ntp = mesh.shape["tp"]

    def pp(v, j):
        return lax.ppermute(v, "tp", [(i, i ^ j) for i in range(ntp)])

    def grad_dx(dn, xl, gf, dresl):
        xf = xl.astype(F32)
        rs = lax.rsqrt(jnp.mean(xf * xf, axis=-1, keepdims=True) + EPS)
        nh = xf * rs
        gdn = gf * dn
        dx = dresl.astype(F32) + rs * (gdn - nh * jnp.mean(nh * gdn, axis=-1, keepdims=True))
        dg = jnp.sum(dn * nh, axis=0)
        return dx.astype(BF16), dg

    def body(ids, E, g, W, du, dres):
        vs, d = E.shape
        nk, t = ids.shape
        ts = t // ntp
        tl = nk * ts
        nt = nk * t
        fs = W.shape[1]
        h = d // 2
        me = lax.axis_index("tp")
        core = me & 1
        chip = me >> 1
        lo = me * vs
        gf = g.astype(F32)
        i32 = jnp.int32
        big = i32(1 << 20)

        ws = pp(W, 1)
        duv = du.reshape(nk, ntp // 2, 2, ts, fs)
        dum = lax.dynamic_index_in_dim(duv, core, 2, keepdims=False)
        dus = pp(lax.dynamic_index_in_dim(duv, 1 - core, 2, keepdims=False), 1)

        def part(k, c0):
            q = chip ^ k
            a = lax.dynamic_index_in_dim(dum, q, 1, keepdims=False).reshape(tl, fs)
            b = lax.dynamic_index_in_dim(dus, q, 1, keepdims=False).reshape(tl, fs)
            pa = rnd(lax.dot_general(a, W[c0 : c0 + h], C1, preferred_element_type=F32))
            pb = rnd(lax.dot_general(b, ws[c0 : c0 + h], C1, preferred_element_type=F32))
            return pa + pb

        with jax.named_scope("d3"):
            r2 = pp(part(3, 0), 2)
            r1 = pp(part(3, h), 4)
        with jax.named_scope("d1"):
            ax = pp(part(1, 0), 2)
            ay = pp(part(2, h), 4)

        idf = ids.reshape(nt)
        own = idf // vs
        tok = jnp.arange(nt, dtype=i32)
        eq = idf[:, None] == idf[None, :]
        first = jnp.min(jnp.where(eq, tok[:, None], big), axis=0)
        isf = first == tok
        slot = jnp.sum(
            (isf[:, None] & (own[:, None] == own[None, :]) & (tok[:, None] < first[None, :])).astype(i32), axis=0
        )
        idl = ids.reshape(nk, ntp, ts).transpose(1, 0, 2).reshape(ntp, tl)
        ownl = idl // vs
        tkl = jnp.arange(tl, dtype=i32)
        eql = idl[:, :, None] == idl[:, None, :]
        firstl = jnp.min(jnp.where(eql, tkl[None, :, None], big), axis=1)
        isfl = firstl == tkl[None, :]
        slotl = jnp.sum(
            (
                isfl[:, :, None] & (ownl[:, :, None] == ownl[:, None, :]) & (tkl[None, :, None] < firstl[:, None, :])
            ).astype(i32),
            axis=1,
        )
        over = (jnp.max(slot) >= CX) | (jnp.max(slotl) >= CD - 1)

        row_of = jnp.max(
            jnp.where(
                (own == me)[:, None] & (slot[:, None] == jnp.arange(CX, dtype=i32)[None, :]),
                (idf - lo)[:, None],
                -1,
            ),
            axis=0,
        )
        ohe = (row_of[:, None] == lax.broadcasted_iota(i32, (CX, vs), 1)).astype(BF16)
        xc = jnp.dot(ohe, E, preferred_element_type=F32).astype(BF16)
        hc = CX // 2
        with jax.named_scope("x1"):
            px = pp(xc, 2)
            py = pp(xc, 4)
        with jax.named_scope("x2"):
            dlo = pp(px[:hc], 4)
            dhi = pp(py[hc:], 2)
        with jax.named_scope("xs"):
            sib = [pp(v, 1) for v in (xc, px, py, jnp.concatenate([dlo, dhi], axis=0))]
        xall = jnp.concatenate([xc, px, py, dlo, dhi] + sib, axis=0)
        xf = xall.astype(F32)
        rs = lax.rsqrt(jnp.mean(xf * xf, axis=-1, keepdims=True) + EPS)
        nc = (xf * rs * gf).astype(BF16)
        gpos = (((own ^ me) & 1) * (ntp // 2) + ((own ^ me) >> 1)) * CX + slot
        oh = (gpos[:, None] == lax.broadcasted_iota(i32, (nt, ntp * CX), 1)).astype(BF16)
        with jax.named_scope("mm"):
            n = jnp.dot(oh, nc, preferred_element_type=F32).astype(BF16)
            uc = jnp.dot(nc, W, preferred_element_type=F32).astype(BF16)
            u = jnp.dot(oh, uc, preferred_element_type=F32).astype(BF16).reshape(nk, t, fs)
            dW = lax.dot_general(n, du.reshape(nt, fs), C0, preferred_element_type=F32)
            ohl = lax.dynamic_slice_in_dim(oh.reshape(nk, t, ntp * CX), me * ts, ts, 1).reshape(tl, ntp * CX)
            xl = jnp.dot(ohl, xall, preferred_element_type=F32).astype(BF16)

        with jax.named_scope("d2"):
            by = pp(part(2, 0) + r2, 4)
            bx = pp(part(1, h) + r1, 2)
        dn = jnp.concatenate([part(0, 0) + ax + by, part(0, h) + ay + bx], axis=1)

        dxb, dgp = grad_dx(dn, xl, gf, dres.reshape(tl, d))

        om = lax.dynamic_index_in_dim(ownl, me, 0, keepdims=False)
        sm = lax.dynamic_index_in_dim(slotl, me, 0, keepdims=False)
        pm = (om ^ me) * CD + sm
        ohm = (lax.broadcasted_iota(i32, (ntp * CD, tl), 0) == pm[None, :]).astype(BF16)
        rows = jnp.dot(ohm, dxb, preferred_element_type=F32).reshape(ntp, CD, d)
        rows = jnp.where(lax.broadcasted_iota(i32, (1, CD, 1), 1) == CD - 1, dgp[None, None, :], rows)
        with jax.named_scope("e"):
            got = jnp.stack([rows[0]] + [pp(rows[j], j) for j in range(1, ntp)])
        dg = jnp.sum(jnp.take(got[:, CD - 1], jnp.arange(ntp, dtype=i32) ^ me, axis=0), axis=0)
        vr = jnp.max(
            jnp.where(
                (ownl == me)[:, :, None] & (slotl[:, :, None] == jnp.arange(CD, dtype=i32)[None, None, :]),
                (idl - lo)[:, :, None],
                -1,
            ),
            axis=1,
        )
        vr = jnp.take(vr, jnp.arange(ntp, dtype=i32) ^ me, axis=0)
        vr = jnp.where(jnp.arange(CD, dtype=i32)[None, :] == CD - 1, -1, vr).reshape(ntp * CD)
        got = got.reshape(ntp * CD, d)
        s1 = rnd(got)
        e1 = got - s1
        s2 = rnd(e1)
        s3 = e1 - s2
        sp = jnp.concatenate([s1.astype(BF16), s2.astype(BF16), s3.astype(BF16)], axis=0)
        vr3 = jnp.concatenate([vr, vr, vr], axis=0)
        ohd = (lax.broadcasted_iota(i32, (vs, 3 * ntp * CD), 0) == vr3[None, :]).astype(BF16)
        dE = jnp.dot(ohd, sp, preferred_element_type=F32)
        fast = (u, xl.reshape(nk, ts, d), dE, dW, dg)

        def slow(_):
            def step(k, st):
                u, x_, dE, dW, dg = st
                ik = lax.dynamic_index_in_dim(ids, k, 0, keepdims=False)
                duk = lax.dynamic_index_in_dim(du, k, 0, keepdims=False)
                oh = (lax.broadcasted_iota(i32, (vs, t), 0) == (ik - lo)[None, :]).astype(BF16)
                x = lax.dot_general(oh, E, C0, preferred_element_type=F32).astype(BF16)
                for j in (1, 2, 4):
                    x = x + pp(x, j)
                xf = x.astype(F32)
                rs = lax.rsqrt(jnp.mean(xf * xf, axis=-1, keepdims=True) + EPS)
                n = (xf * rs * gf).astype(BF16)
                uk = jnp.dot(n, W, preferred_element_type=F32).astype(BF16)
                dW = dW + lax.dot_general(n, duk, C0, preferred_element_type=F32)
                xl = lax.dynamic_slice_in_dim(x, me * ts, ts, 0)
                p = lax.dot_general(duk, W, C1, preferred_element_type=F32).astype(BF16).reshape(ntp, ts, d)
                dn = jnp.zeros((ts, d), F32)
                for j in range(ntp):
                    q = lax.dynamic_index_in_dim(p, me ^ j, 0, keepdims=False)
                    dn = dn + (pp(q, j) if j else q).astype(F32)
                dxb, dgk = grad_dx(dn, xl, gf, lax.dynamic_index_in_dim(dres, k, 0, keepdims=False))
                dxa = lax.dynamic_update_slice_in_dim(jnp.zeros((t, d), BF16), dxb, me * ts, 0)
                for j in (1, 2, 4):
                    dxa = dxa + pp(dxa, j)
                dE = dE + jnp.dot(oh, dxa, preferred_element_type=F32)
                u = lax.dynamic_update_index_in_dim(u, uk, k, 0)
                x_ = lax.dynamic_update_index_in_dim(x_, xl, k, 0)
                return u, x_, dE, dW, dg + dgk

            u, x_, dE, dW, dg = lax.fori_loop(0, nk, step, jax.tree.map(jnp.zeros_like, fast))
            for j in (1, 2, 4):
                dg = dg + pp(dg, j)
            return u, x_, dE, dW, dg

        return lax.while_loop(lambda s: s[0], lambda s: (jnp.bool_(False), slow(s[1])), (over, fast))[1]

    return jax.shard_map(
        body,
        mesh=mesh,
        in_specs=(P("dp", None), P("tp", None), P(None), P(None, "tp"), P("dp", None, "tp"), P("dp", "tp", None)),
        out_specs=(P("dp", None, "tp"), P("dp", "tp", None), P(("dp", "tp"), None), P("dp", "tp"), P("dp")),
        check_vma=False,
    )
```
